32 devices in a mesh: south: 2 (over core), east: 4 (over z), down: 2 (over x), ens: 2 (over y).
Axes of the slice: x: 2, y: 2, z: 4, core: 2. Of those that a mesh axis runs over, the one named last changes fastest.
Arguments:
- density: float32 [16, 128, 128, 128], P(('ens', 'south'), 'east', 'down'), parts along dimension 0, may hold values from 0.2 to 1.8
- flow_j: float32 [16, 128, 128, 128], P(('ens', 'south'), 'east', 'down'), parts along dimension 0, may hold values from -0.3 to 0.3
- flow_i: float32 [16, 128, 128, 128], P(('ens', 'south'), 'east', 'down'), parts along dimension 0, may hold values from -0.3 to 0.3
- flow_k: float32 [16, 128, 128, 128], P(('ens', 'south'), 'east', 'down'), parts along dimension 0, may hold values from -0.3 to 0.3
Outputs:
- density_end: float32 [16, 128, 128, 128], P(('ens', 'south'), 'east', 'down'), parts along dimension 0
The draws below stay inside these ranges and needn't reach their ends.
There are 2 independent parts, one for each index of `ens`. The reference program is written for one: setup_inputs(seed, part) draws one part's arguments, and reference() takes and returns one part's arrays. A program takes and returns all parts, laid end to end along the dimension named above; each array names one. Nothing has to cross between parts.
All inputs are finite; a program needn't handle non-finite values.
Results may differ from the reference program's by a relative error of at most 0.00002.
Values sent between devices are 32-bit elements; how exact they have to be, the bound alone decides.
A program may use at most 192 MiB of HBM per device.

```python
import jax
import jax.numpy as jnp
from jax import lax

GRID_J = 8
GRID_I = 128
GRID_K = 128
SPECIES = 128
STEPS = 3


def levels(own_key, extent, split, low, top_value):
    def one(axis_at, blocks):
        draws = jax.random.uniform(jax.random.fold_in(jax.random.fold_in(own_key, 6), axis_at), (blocks,), jnp.float32, low / len(split), top_value / len(split))
        return jnp.repeat(jnp.exp(draws), extent[axis_at] // blocks).reshape((-1,) + (1,) * (len(extent) - axis_at - 1))

    gain = one(*split[0])
    for cut in split[1:]:
        gain = gain * one(*cut)
    return gain


def setup_inputs(seed: int = 0, part: int = 0) -> dict:
    keys = jax.random.split(jax.random.key(seed), 5)
    part_keys = jax.random.split(jax.random.fold_in(keys[4], part), 5)
    density = jnp.clip(0.2 + 1.5999999 * jax.random.uniform(part_keys[0], (GRID_J, GRID_I, GRID_K, SPECIES), jnp.float32) ** levels(part_keys[0], (GRID_J, GRID_I, GRID_K, SPECIES), ((0, 2), (1, 4), (2, 2)), -0.2, 0.2), 0.2, 1.8)
    flow_j = jnp.clip(jax.random.uniform(part_keys[1], (GRID_J, GRID_I, GRID_K, SPECIES), jnp.float32, -0.3, 0.3) * levels(part_keys[1], (GRID_J, GRID_I, GRID_K, SPECIES), ((0, 2), (1, 4), (2, 2)), -0.4, 0.0), -0.3, 0.3)
    flow_i = jnp.clip(jax.random.uniform(part_keys[2], (GRID_J, GRID_I, GRID_K, SPECIES), jnp.float32, -0.3, 0.3) * levels(part_keys[2], (GRID_J, GRID_I, GRID_K, SPECIES), ((0, 2), (1, 4), (2, 2)), -0.4, 0.0), -0.3, 0.3)
    flow_k = jnp.clip(jax.random.uniform(part_keys[3], (GRID_J, GRID_I, GRID_K, SPECIES), jnp.float32, -0.3, 0.3) * levels(part_keys[3], (GRID_J, GRID_I, GRID_K, SPECIES), ((0, 2), (1, 4), (2, 2)), -0.4, 0.0), -0.3, 0.3)
    return dict(density=density, flow_j=flow_j, flow_i=flow_i, flow_k=flow_k)


def inner_cells(values, dims):
    for dim in dims:
        values = lax.slice_in_dim(values, 1, values.shape[dim] - 1, axis=dim)
    return values


def side_cells(values, dim, start, dims):
    others = [other for other in dims if other != dim]
    values = inner_cells(values, others)
    return lax.slice_in_dim(values, start, start + values.shape[dim] - 2, axis=dim)


def advance(padded, flow_j, flow_i, flow_k):
    middle = inner_cells(padded, (0, 1, 2))
    lower = [side_cells(padded, dim, 0, (0, 1, 2)) for dim in (0, 1, 2)]
    upper = [side_cells(padded, dim, 2, (0, 1, 2)) for dim in (0, 1, 2)]
    slopes = [above - below for above, below in zip(upper, lower)]
    smooth_rate = 0.05
    spread = lower[0] + upper[0] + lower[1] + upper[1] + lower[2] + upper[2] - 6.0 * middle
    return middle - flow_j * slopes[0] - flow_i * slopes[1] - flow_k * slopes[2] + smooth_rate * spread


def reference(density, flow_j, flow_i, flow_k):
    for step in range(STEPS):
        density = advance(jnp.pad(density, ((1, 1), (1, 1), (1, 1), (0, 0)), mode="constant"), flow_j, flow_i, flow_k)
    return density
```

```python
import functools

import jax
import jax.numpy as jnp
from jax import lax
from jax.experimental import pallas as pl
from jax.experimental.pallas import tpu as pltpu
from jax.sharding import PartitionSpec as P

STEPS = 3
TILE = 8
MESH = pl.DeviceIdType.MESH


def divisor(total, most):
    return max(d for d in range(1, most + 1) if total % d == 0)


def kernel(
    counts, density, flow_j, flow_i, flow_k, out,
    field, fj, fi, fk, pack, land,
    load_sem, flow_sem, isend, irecv, ksend, krecv, jsend, jrecv,
):
    nj, ni, nk, lanes = density.shape
    n_south, n_east, n_down = counts
    south, east, down = (lax.axis_index(a) for a in ("south", "east", "down"))
    has = {
        ("south", 0): (n_south > 1, south > 0),
        ("south", 1): (n_south > 1, south < n_south - 1),
        ("east", 0): (n_east > 1, east > 0),
        ("east", 1): (n_east > 1, east < n_east - 1),
        ("down", 0): (n_down > 1, down > 0),
        ("down", 1): (n_down > 1, down < n_down - 1),
    }
    index = {"south": south, "east": east, "down": down}

    def neighbour(axis, side):
        return {axis: index[axis] + (1 if side else -1)}

    def when_has(axis, side, act):
        static, dynamic = has[axis, side]
        if static:
            pl.when(dynamic)(act)

    def when_edge(axis, side, act):
        static, dynamic = has[axis, side]
        if static:
            pl.when(jnp.logical_not(dynamic))(act)
        else:
            act()

    middle = [j for j in range(nj) if 0 < j < nj - 1]
    outer = [j for j in range(nj) if not 0 < j < nj - 1]
    inner_order = middle + outer
    inside_k = pl.ds(TILE, nk)

    def load(j):
        return pltpu.make_async_copy(
            density.at[j], field.at[0, j + 1, pl.ds(1, ni), inside_k], load_sem.at[j]
        )

    def load_flow(j, d):
        source, target = ((flow_j, fj), (flow_i, fi), (flow_k, fk))[d]
        return pltpu.make_async_copy(source.at[j], target.at[j], flow_sem.at[d, j])

    for j in outer + middle:
        load(j).start()
    for j in inner_order:
        for d in range(3):
            load_flow(j, d).start()

    barrier = pltpu.get_barrier_semaphore()
    for axis, side in has:
        def greet(axis=axis, side=side):
            pl.semaphore_signal(
                barrier, inc=1, device_id=neighbour(axis, side), device_id_type=MESH
            )
        when_has(axis, side, greet)

    def zero_plane(ref_at):
        def act():
            for s in range(STEPS):
                ref_at(s)
        return act

    for side in range(2):
        def zero_j(s, side=side):
            @pl.loop(0, ni)
            def _(i):
                field[s, (nj + 1) * side, i + 1, inside_k, :] = jnp.zeros((nk, lanes), jnp.float32)

        def zero_i(s, side=side):
            for j in range(nj):
                field[s, j + 1, (ni + 1) * side, inside_k, :] = jnp.zeros((nk, lanes), jnp.float32)

        def zero_k(s, side=side):
            row = TILE + nk if side else TILE - 1
            for j in range(nj):
                @pl.loop(0, ni, unroll=8)
                def _(i):
                    field[s, j + 1, i + 1, pl.ds(row, 1), :] = jnp.zeros((1, lanes), jnp.float32)

        when_edge("south", side, zero_plane(zero_j))
        when_edge("east", side, zero_plane(zero_i))
        when_edge("down", side, zero_plane(zero_k))

    pl.semaphore_wait(barrier, sum(jnp.where(d, 1, 0) for s, d in has.values() if s))

    def copy_i(s, side, j):
        face = ni if side else 1
        halo = 0 if side else ni + 1
        return pltpu.make_async_remote_copy(
            src_ref=field.at[s, j + 1, face, inside_k],
            dst_ref=field.at[s, j + 1, halo, inside_k],
            send_sem=isend.at[s, side, j],
            recv_sem=irecv.at[s, 1 - side, j],
            device_id=neighbour("east", side),
            device_id_type=MESH,
        )

    def copy_k(s, side, j):
        return pltpu.make_async_remote_copy(
            src_ref=pack.at[s, side, j],
            dst_ref=land.at[s, 1 - side, j],
            send_sem=ksend.at[s, side, j],
            recv_sem=krecv.at[s, 1 - side, j],
            device_id=neighbour("down", side),
            device_id_type=MESH,
        )

    def copy_j(s, side):
        face = nj if side else 1
        halo = 0 if side else nj + 1
        return pltpu.make_async_remote_copy(
            src_ref=field.at[s, face, pl.ds(1, ni), inside_k],
            dst_ref=field.at[s, halo, pl.ds(1, ni), inside_k],
            send_sem=jsend.at[s, side],
            recv_sem=jrecv.at[s, 1 - side],
            device_id=neighbour("south", side),
            device_id_type=MESH,
        )

    first = jnp.where(south == 0, 1, 0) if n_south > 1 else 0

    def chunk(t):
        return first * (nj - 1 - t) + (1 - first) * t

    def send_chunk(s, t):
        j = chunk(t)
        for side in range(2):
            when_has("east", side, lambda side=side: copy_i(s, side, j).start())
        if n_south > 1 and t == 0:
            pl.when(south == 0)(lambda: copy_j(s, 1).start())
            pl.when(south > 0)(lambda: copy_j(s, 0).start())
        if n_south > 2 and t == nj - 1:
            pl.when((south > 0) & (south < n_south - 1))(lambda: copy_j(s, 1).start())
        for side in range(2):
            def send_k(side=side):
                row = TILE + nk - 1 if side else TILE
                for i in range(ni):
                    pack[s, side, j, pl.ds(i, 1), :] = field[s, j + 1, i + 1, pl.ds(row, 1), :]
                copy_k(s, side, j).start()
            when_has("down", side, send_k)

    def block(s, j, i, size_i, k, size_k):
        def at(dj, di, dk):
            return field[
                s, j + 1 + dj, pl.ds(i + 1 + di, size_i), pl.ds(TILE + k + dk, size_k), :
            ]

        cells = (j, pl.ds(i, size_i), pl.ds(k, size_k), slice(None))
        lower = [at(-1, 0, 0), at(0, -1, 0), at(0, 0, -1)]
        upper = [at(1, 0, 0), at(0, 1, 0), at(0, 0, 1)]
        total = (lower[0] + upper[0]) + (lower[1] + upper[1]) + (lower[2] + upper[2])
        drift = (
            fj[cells] * (upper[0] - lower[0])
            + fi[cells] * (upper[1] - lower[1])
            + fk[cells] * (upper[2] - lower[2])
        )
        value = (0.7 * at(0, 0, 0) + 0.05 * total) - drift
        if s + 1 < STEPS:
            field[s + 1, j + 1, pl.ds(i + 1, size_i), pl.ds(TILE + k, size_k), :] = value
        else:
            out[cells] = value

    for j in range(nj):
        load(j).wait()
    for t in range(nj):
        send_chunk(0, t)

    wide = divisor(ni - 2, 2)
    tall = divisor(ni - 2, 10)
    for s in range(STEPS):
        for at_j, j in enumerate(inner_order):
            if s == 0:
                for d in range(3):
                    load_flow(j, d).wait()
            if at_j == len(middle):
                for side in range(2):
                    when_has("south", side, lambda side=side: copy_j(s, 1 - side).wait_recv())

            @pl.loop(0, (ni - 2) // wide)
            def _(b, j=j):
                block(s, j, 1 + b * wide, wide, TILE, nk - 2 * TILE)

        for t in range(nj):
            j = chunk(t)
            for side in range(2):
                def unpack(side=side):
                    copy_k(s, 1 - side, j).wait_recv()
                    row = TILE + nk if side else TILE - 1
                    for i in range(ni):
                        field[s, j + 1, i + 1, pl.ds(row, 1), :] = land[s, side, j, pl.ds(i, 1), :]
                when_has("down", side, unpack)

            @pl.loop(0, (ni - 2) // tall)
            def _(b):
                block(s, j, 1 + b * tall, tall, 0, TILE)
                block(s, j, 1 + b * tall, tall, nk - TILE, TILE)

            for side in range(2):
                when_has("east", side, lambda side=side: copy_i(s, 1 - side, j).wait_recv())
            block(s, j, 0, 1, 0, nk)
            block(s, j, ni - 1, 1, 0, nk)
            if s + 1 < STEPS:
                send_chunk(s + 1, t)

    for s in range(STEPS):
        for side in range(2):
            when_has("south", side, lambda side=side: copy_j(s, side).wait_send())
            for j in range(nj):
                when_has("east", side, lambda side=side, j=j: copy_i(s, side, j).wait_send())
                when_has("down", side, lambda side=side, j=j: copy_k(s, side, j).wait_send())


def per_device(counts, density, flow_j, flow_i, flow_k):
    nj, ni, nk, lanes = density.shape
    f32 = jnp.float32
    dma = pltpu.SemaphoreType.DMA
    return pl.pallas_call(
        functools.partial(kernel, counts),
        out_shape=jax.ShapeDtypeStruct(density.shape, f32),
        in_specs=[pl.BlockSpec(memory_space=pl.ANY)] * 4,
        out_specs=pl.BlockSpec(memory_space=pltpu.VMEM),
        scratch_shapes=[
            pltpu.VMEM((STEPS, nj + 2, ni + 2, nk + 2 * TILE, lanes), f32),
            pltpu.VMEM((nj, ni, nk, lanes), f32),
            pltpu.VMEM((nj, ni, nk, lanes), f32),
            pltpu.VMEM((nj, ni, nk, lanes), f32),
            pltpu.VMEM((STEPS, 2, nj, ni, lanes), f32),
            pltpu.VMEM((STEPS, 2, nj, ni, lanes), f32),
            dma((nj,)),
            dma((3, nj)),
            dma((STEPS, 2, nj)),
            dma((STEPS, 2, nj)),
            dma((STEPS, 2, nj)),
            dma((STEPS, 2, nj)),
            dma((STEPS, 2)),
            dma((STEPS, 2)),
        ],
        compiler_params=pltpu.CompilerParams(
            collective_id=0, has_side_effects=True, vmem_limit_bytes=60 * 1024 * 1024
        ),
    )(density, flow_j, flow_i, flow_k)


def solution(mesh):
    spec = P(("ens", "south"), "east", "down", None)
    counts = tuple(mesh.shape[a] for a in ("south", "east", "down"))
    return jax.shard_map(
        functools.partial(per_device, counts),
        mesh=mesh,
        in_specs=(spec,) * 4,
        out_specs=spec,
        check_vma=False,
    )
```

```python
import functools

import jax
import jax.numpy as jnp
from jax import lax
from jax.experimental import pallas as pl
from jax.experimental.pallas import tpu as pltpu
from jax.sharding import PartitionSpec as P

STEPS = 3
TILE = 8
MESH = pl.DeviceIdType.MESH


def divisor(total, most):
    return max(d for d in range(1, most + 1) if total % d == 0)


def kernel(
    counts, density, flow_j, flow_i, flow_k, out,
    field, fj, fi, fk, pack, land,
    load_sem, flow_sem, isend, irecv, ksend, krecv, jsend, jrecv,
):
    nj, ni, nk, lanes = density.shape
    n_south, n_east, n_down = counts
    south, east, down = (lax.axis_index(a) for a in ("south", "east", "down"))
    has = {
        ("south", 0): (n_south > 1, south > 0),
        ("south", 1): (n_south > 1, south < n_south - 1),
        ("east", 0): (n_east > 1, east > 0),
        ("east", 1): (n_east > 1, east < n_east - 1),
        ("down", 0): (n_down > 1, down > 0),
        ("down", 1): (n_down > 1, down < n_down - 1),
    }
    index = {"south": south, "east": east, "down": down}

    def neighbour(axis, side):
        return {axis: index[axis] + (1 if side else -1)}

    def when_has(axis, side, act):
        static, dynamic = has[axis, side]
        if static:
            pl.when(dynamic)(act)

    def when_edge(axis, side, act):
        static, dynamic = has[axis, side]
        if static:
            pl.when(jnp.logical_not(dynamic))(act)
        else:
            act()

    middle = [j for j in range(nj) if 0 < j < nj - 1]
    outer = [j for j in range(nj) if not 0 < j < nj - 1]
    inner_order = middle + outer
    inside_k = pl.ds(TILE, nk)

    def load(j):
        return pltpu.make_async_copy(
            density.at[j], field.at[0, j + 1, pl.ds(1, ni), inside_k], load_sem.at[j]
        )

    def load_flow(j, d):
        source, target = ((flow_j, fj), (flow_i, fi), (flow_k, fk))[d]
        return pltpu.make_async_copy(source.at[j], target.at[j], flow_sem.at[d, j])

    for j in outer + middle:
        load(j).start()
    for j in inner_order:
        for d in range(3):
            load_flow(j, d).start()

    barrier = pltpu.get_barrier_semaphore()
    for axis, side in has:
        def greet(axis=axis, side=side):
            pl.semaphore_signal(
                barrier, inc=1, device_id=neighbour(axis, side), device_id_type=MESH
            )
        when_has(axis, side, greet)

    def zero_plane(ref_at):
        def act():
            for s in range(STEPS):
                ref_at(s)
        return act

    for side in range(2):
        def zero_j(s, side=side):
            @pl.loop(0, ni)
            def _(i):
                field[s, (nj + 1) * side, i + 1, inside_k, :] = jnp.zeros((nk, lanes), jnp.float32)

        def zero_i(s, side=side):
            for j in range(nj):
                field[s, j + 1, (ni + 1) * side, inside_k, :] = jnp.zeros((nk, lanes), jnp.float32)

        def zero_k(s, side=side):
            row = TILE + nk if side else TILE - 1
            for j in range(nj):
                @pl.loop(0, ni, unroll=8)
                def _(i):
                    field[s, j + 1, i + 1, pl.ds(row, 1), :] = jnp.zeros((1, lanes), jnp.float32)

        when_edge("south", side, zero_plane(zero_j))
        when_edge("east", side, zero_plane(zero_i))
        when_edge("down", side, zero_plane(zero_k))

    pl.semaphore_wait(barrier, sum(jnp.where(d, 1, 0) for s, d in has.values() if s))

    def copy_i(s, side, j):
        face = ni if side else 1
        halo = 0 if side else ni + 1
        return pltpu.make_async_remote_copy(
            src_ref=field.at[s, j + 1, face, inside_k],
            dst_ref=field.at[s, j + 1, halo, inside_k],
            send_sem=isend.at[s, side, j],
            recv_sem=irecv.at[s, 1 - side, j],
            device_id=neighbour("east", side),
            device_id_type=MESH,
        )

    def copy_k(s, side, j):
        return pltpu.make_async_remote_copy(
            src_ref=pack.at[s, side, j],
            dst_ref=land.at[s, 1 - side, j],
            send_sem=ksend.at[s, side, j],
            recv_sem=krecv.at[s, 1 - side, j],
            device_id=neighbour("down", side),
            device_id_type=MESH,
        )

    def copy_j(s, side):
        face = nj if side else 1
        halo = 0 if side else nj + 1
        return pltpu.make_async_remote_copy(
            src_ref=field.at[s, face, pl.ds(1, ni), inside_k],
            dst_ref=field.at[s, halo, pl.ds(1, ni), inside_k],
            send_sem=jsend.at[s, side],
            recv_sem=jrecv.at[s, 1 - side],
            device_id=neighbour("south", side),
            device_id_type=MESH,
        )

    first = jnp.where(south == 0, 1, 0) if n_south > 1 else 0

    def chunk(t):
        return first * (nj - 1 - t) + (1 - first) * t

    def send_chunk(s, t):
        j = chunk(t)
        for side in range(2):
            when_has("east", side, lambda side=side: copy_i(s, side, j).start())
        if n_south > 1 and t == 0:
            pl.when(south == 0)(lambda: copy_j(s, 1).start())
            pl.when(south > 0)(lambda: copy_j(s, 0).start())
        if n_south > 2 and t == nj - 1:
            pl.when((south > 0) & (south < n_south - 1))(lambda: copy_j(s, 1).start())
        for side in range(2):
            def send_k(side=side):
                row = TILE + nk - 1 if side else TILE
                for i in range(ni):
                    pack[s, side, j, pl.ds(i, 1), :] = field[s, j + 1, i + 1, pl.ds(row, 1), :]
                copy_k(s, side, j).start()
            when_has("down", side, send_k)

    def block(s, j, i, size_i, k, size_k):
        def at(dj, di, dk):
            return field[
                s, j + 1 + dj, pl.ds(i + 1 + di, size_i), pl.ds(TILE + k + dk, size_k), :
            ]

        cells = (j, pl.ds(i, size_i), pl.ds(k, size_k), slice(None))
        lower = [at(-1, 0, 0), at(0, -1, 0), at(0, 0, -1)]
        upper = [at(1, 0, 0), at(0, 1, 0), at(0, 0, 1)]
        total = (lower[0] + upper[0]) + (lower[1] + upper[1]) + (lower[2] + upper[2])
        drift = (
            fj[cells] * (upper[0] - lower[0])
            + fi[cells] * (upper[1] - lower[1])
            + fk[cells] * (upper[2] - lower[2])
        )
        value = (0.7 * at(0, 0, 0) + 0.05 * total) - drift
        if s + 1 < STEPS:
            field[s + 1, j + 1, pl.ds(i + 1, size_i), pl.ds(TILE + k, size_k), :] = value
        else:
            out[cells] = value

    for j in range(nj):
        load(j).wait()
    for t in range(nj):
        send_chunk(0, t)

    wide = divisor(ni - 2, 2)
    tall = divisor(ni - 2, 10)
    for s in range(STEPS):
        for at_j, j in enumerate(inner_order):
            if s == 0:
                for d in range(3):
                    load_flow(j, d).wait()
            if at_j == len(middle):
                for side in range(2):
                    when_has("south", side, lambda side=side: copy_j(s, 1 - side).wait_recv())

            @pl.loop(0, (ni - 2) // wide)
            def _(b, j=j):
                block(s, j, 1 + b * wide, wide, TILE, nk - 2 * TILE)

        for t in range(nj):
            j = chunk(t)
            for side in range(2):
                def unpack(side=side):
                    copy_k(s, 1 - side, j).wait_recv()
                    row = TILE + nk if side else TILE - 1
                    for i in range(ni):
                        field[s, j + 1, i + 1, pl.ds(row, 1), :] = land[s, side, j, pl.ds(i, 1), :]
                when_has("down", side, unpack)

            @pl.loop(0, (ni - 2) // tall)
            def _(b):
                block(s, j, 1 + b * tall, tall, 0, TILE)
                block(s, j, 1 + b * tall, tall, nk - TILE, TILE)

            for side in range(2):
                when_has("east", side, lambda side=side: copy_i(s, 1 - side, j).wait_recv())
            block(s, j, 0, 1, 0, nk)
            block(s, j, ni - 1, 1, 0, nk)
            if s + 1 < STEPS:
                send_chunk(s + 1, t)

    for s in range(STEPS):
        for side in range(2):
            when_has("south", side, lambda side=side: copy_j(s, side).wait_send())
            for j in range(nj):
                when_has("east", side, lambda side=side, j=j: copy_i(s, side, j).wait_send())
                when_has("down", side, lambda side=side, j=j: copy_k(s, side, j).wait_send())


def per_device(counts, density, flow_j, flow_i, flow_k):
    nj, ni, nk, lanes = density.shape
    f32 = jnp.float32
    dma = pltpu.SemaphoreType.DMA
    return pl.pallas_call(
        functools.partial(kernel, counts),
        out_shape=pltpu.VMEM(density.shape, f32),
        in_specs=[pl.BlockSpec(memory_space=pl.ANY)] * 4,
        out_specs=pl.BlockSpec(memory_space=pltpu.VMEM),
        scratch_shapes=[
            pltpu.VMEM((STEPS, nj + 2, ni + 2, nk + 2 * TILE, lanes), f32),
            pltpu.VMEM((nj, ni, nk, lanes), f32),
            pltpu.VMEM((nj, ni, nk, lanes), f32),
            pltpu.VMEM((nj, ni, nk, lanes), f32),
            pltpu.VMEM((STEPS, 2, nj, ni, lanes), f32),
            pltpu.VMEM((STEPS, 2, nj, ni, lanes), f32),
            dma((nj,)),
            dma((3, nj)),
            dma((STEPS, 2, nj)),
            dma((STEPS, 2, nj)),
            dma((STEPS, 2, nj)),
            dma((STEPS, 2, nj)),
            dma((STEPS, 2)),
            dma((STEPS, 2)),
        ],
        compiler_params=pltpu.CompilerParams(
            collective_id=0, has_side_effects=True, vmem_limit_bytes=58 * 1024 * 1024
        ),
    )(density, flow_j, flow_i, flow_k)


def solution(mesh):
    spec = P(("ens", "south"), "east", "down", None)
    counts = tuple(mesh.shape[a] for a in ("south", "east", "down"))
    return jax.shard_map(
        functools.partial(per_device, counts),
        mesh=mesh,
        in_specs=(spec,) * 4,
        out_specs=spec,
        check_vma=False,
    )
```

```python
import functools

import jax
import jax.numpy as jnp
from jax import lax
from jax.experimental import pallas as pl
from jax.experimental.pallas import tpu as pltpu
from jax.sharding import PartitionSpec as P

STEPS = 3
TILE = 8
MESH = pl.DeviceIdType.MESH


def divisor(total, most):
    return max(d for d in range(1, most + 1) if total % d == 0)


def kernel(
    counts, density, flow_j, flow_i, flow_k, out,
    field, fj, fi, fk, pack, land,
    load_sem, flow_sem, isend, irecv, ksend, krecv, jsend, jrecv,
):
    nj, ni, nk, lanes = density.shape
    n_south, n_east, n_down = counts
    south, east, down = (lax.axis_index(a) for a in ("south", "east", "down"))
    has = {
        ("south", 0): (n_south > 1, south > 0),
        ("south", 1): (n_south > 1, south < n_south - 1),
        ("east", 0): (n_east > 1, east > 0),
        ("east", 1): (n_east > 1, east < n_east - 1),
        ("down", 0): (n_down > 1, down > 0),
        ("down", 1): (n_down > 1, down < n_down - 1),
    }
    index = {"south": south, "east": east, "down": down}

    def neighbour(axis, side):
        return {axis: index[axis] + (1 if side else -1)}

    def when_has(axis, side, act):
        static, dynamic = has[axis, side]
        if static:
            pl.when(dynamic)(act)

    def when_edge(axis, side, act):
        static, dynamic = has[axis, side]
        if static:
            pl.when(jnp.logical_not(dynamic))(act)
        else:
            act()

    middle = [j for j in range(nj) if 0 < j < nj - 1]
    outer = [j for j in range(nj) if not 0 < j < nj - 1]
    inner_order = middle + outer
    inside_k = pl.ds(TILE, nk)

    def load(j):
        inner = pl.ds(1, ni - 2)
        return pltpu.make_async_copy(
            density.at[j, inner], field.at[0, j + 1, pl.ds(2, ni - 2), inside_k], load_sem.at[j]
        )

    def load_face(side):
        i = (ni - 1) * side
        return pltpu.make_async_copy(
            density.at[:, i], field.at[0, pl.ds(1, nj), i + 1, inside_k], load_sem.at[nj + side]
        )

    def load_flow(j, d):
        source, target = ((flow_j, fj), (flow_i, fi), (flow_k, fk))[d]
        return pltpu.make_async_copy(source.at[j], target.at[j], flow_sem.at[d, j])

    barrier = pltpu.get_barrier_semaphore()
    for axis, side in has:
        def greet(axis=axis, side=side):
            pl.semaphore_signal(
                barrier, inc=1, device_id=neighbour(axis, side), device_id_type=MESH
            )
        when_has(axis, side, greet)

    for side in range(2):
        load_face(side).start()
    for j in outer + middle:
        load(j).start()

    def copy_i(s, side, j):
        face = ni if side else 1
        halo = 0 if side else ni + 1
        return pltpu.make_async_remote_copy(
            src_ref=field.at[s, j + 1, face, inside_k],
            dst_ref=field.at[s, j + 1, halo, inside_k],
            send_sem=isend.at[s, side, j],
            recv_sem=irecv.at[s, 1 - side, j],
            device_id=neighbour("east", side),
            device_id_type=MESH,
        )

    def copy_k(s, side, j):
        return pltpu.make_async_remote_copy(
            src_ref=pack.at[s, side, j],
            dst_ref=land.at[s, 1 - side, j],
            send_sem=ksend.at[s, side, j],
            recv_sem=krecv.at[s, 1 - side, j],
            device_id=neighbour("down", side),
            device_id_type=MESH,
        )

    def copy_j(s, side):
        face = nj if side else 1
        halo = 0 if side else nj + 1
        return pltpu.make_async_remote_copy(
            src_ref=field.at[s, face, pl.ds(1, ni), inside_k],
            dst_ref=field.at[s, halo, pl.ds(1, ni), inside_k],
            send_sem=jsend.at[s, side],
            recv_sem=jrecv.at[s, 1 - side],
            device_id=neighbour("south", side),
            device_id_type=MESH,
        )

    first = jnp.where(south == 0, 1, 0) if n_south > 1 else 0

    def chunk(t):
        return first * (nj - 1 - t) + (1 - first) * t

    def send_i(s, j):
        for side in range(2):
            when_has("east", side, lambda side=side: copy_i(s, side, j).start())

    def send_j(s, t):
        if n_south > 1 and t == 0:
            pl.when(south == 0)(lambda: copy_j(s, 1).start())
            pl.when(south > 0)(lambda: copy_j(s, 0).start())
        if n_south > 2 and t == nj - 1:
            pl.when((south > 0) & (south < n_south - 1))(lambda: copy_j(s, 1).start())

    def send_k(s, j):
        for side in range(2):
            def act(side=side):
                row = TILE + nk - 1 if side else TILE
                for i in range(ni):
                    pack[s, side, j, pl.ds(i, 1), :] = field[s, j + 1, i + 1, pl.ds(row, 1), :]
                copy_k(s, side, j).start()
            when_has("down", side, act)

    def block(s, j, i, size_i, k, size_k):
        def at(dj, di, dk):
            return field[
                s, j + 1 + dj, pl.ds(i + 1 + di, size_i), pl.ds(TILE + k + dk, size_k), :
            ]

        cells = (j, pl.ds(i, size_i), pl.ds(k, size_k), slice(None))
        lower = [at(-1, 0, 0), at(0, -1, 0), at(0, 0, -1)]
        upper = [at(1, 0, 0), at(0, 1, 0), at(0, 0, 1)]
        total = (lower[0] + upper[0]) + (lower[1] + upper[1]) + (lower[2] + upper[2])
        drift = (
            fj[cells] * (upper[0] - lower[0])
            + fi[cells] * (upper[1] - lower[1])
            + fk[cells] * (upper[2] - lower[2])
        )
        value = (0.7 * at(0, 0, 0) + 0.05 * total) - drift
        if s + 1 < STEPS:
            field[s + 1, j + 1, pl.ds(i + 1, size_i), pl.ds(TILE + k, size_k), :] = value
        else:
            out[cells] = value

    pl.semaphore_wait(barrier, sum(jnp.where(d, 1, 0) for s, d in has.values() if s))
    for side in range(2):
        load_face(side).wait()
    for t in range(nj):
        send_i(0, chunk(t))
    for j in middle:
        for d in range(3):
            load_flow(j, d).start()
    for j in range(nj):
        load(j).wait()
    for t in range(nj):
        send_j(0, t)
    for j in outer:
        for d in range(3):
            load_flow(j, d).start()
    for t in range(nj):
        send_k(0, chunk(t))

    def zero_plane(ref_at):
        def act():
            for s in range(STEPS):
                ref_at(s)
        return act

    for side in range(2):
        def zero_j(s, side=side):
            @pl.loop(0, ni)
            def _(i):
                field[s, (nj + 1) * side, i + 1, inside_k, :] = jnp.zeros((nk, lanes), jnp.float32)

        def zero_i(s, side=side):
            for j in range(nj):
                field[s, j + 1, (ni + 1) * side, inside_k, :] = jnp.zeros((nk, lanes), jnp.float32)

        def zero_k(s, side=side):
            row = TILE + nk if side else TILE - 1
            for j in range(nj):
                @pl.loop(0, ni, unroll=8)
                def _(i):
                    field[s, j + 1, i + 1, pl.ds(row, 1), :] = jnp.zeros((1, lanes), jnp.float32)

        when_edge("south", side, zero_plane(zero_j))
        when_edge("east", side, zero_plane(zero_i))
        when_edge("down", side, zero_plane(zero_k))

    wide = divisor(ni - 2, 2)
    tall = divisor(ni - 2, 10)
    for s in range(STEPS):
        for at_j, j in enumerate(inner_order):
            if s == 0:
                for d in range(3):
                    load_flow(j, d).wait()
            if at_j == len(middle):
                for side in range(2):
                    when_has("south", side, lambda side=side: copy_j(s, 1 - side).wait_recv())

            @pl.loop(0, (ni - 2) // wide)
            def _(b, j=j):
                block(s, j, 1 + b * wide, wide, TILE, nk - 2 * TILE)

        for t in range(nj):
            j = chunk(t)
            for side in range(2):
                def unpack(side=side):
                    copy_k(s, 1 - side, j).wait_recv()
                    row = TILE + nk if side else TILE - 1
                    for i in range(ni):
                        field[s, j + 1, i + 1, pl.ds(row, 1), :] = land[s, side, j, pl.ds(i, 1), :]
                when_has("down", side, unpack)

            for side in range(2):
                when_has("east", side, lambda side=side: copy_i(s, 1 - side, j).wait_recv())
            block(s, j, 0, 1, 0, nk)
            block(s, j, ni - 1, 1, 0, nk)
            if s + 1 < STEPS:
                send_i(s + 1, j)

            @pl.loop(0, (ni - 2) // tall)
            def _(b):
                block(s, j, 1 + b * tall, tall, 0, TILE)
                block(s, j, 1 + b * tall, tall, nk - TILE, TILE)

            if s + 1 < STEPS:
                send_j(s + 1, t)
                send_k(s + 1, j)

    for s in range(STEPS):
        for side in range(2):
            when_has("south", side, lambda side=side: copy_j(s, side).wait_send())
            for j in range(nj):
                when_has("east", side, lambda side=side, j=j: copy_i(s, side, j).wait_send())
                when_has("down", side, lambda side=side, j=j: copy_k(s, side, j).wait_send())


def per_device(counts, density, flow_j, flow_i, flow_k):
    nj, ni, nk, lanes = density.shape
    f32 = jnp.float32
    dma = pltpu.SemaphoreType.DMA
    return pl.pallas_call(
        functools.partial(kernel, counts),
        out_shape=pltpu.VMEM(density.shape, f32),
        in_specs=[pl.BlockSpec(memory_space=pl.ANY)] * 4,
        out_specs=pl.BlockSpec(memory_space=pltpu.VMEM),
        scratch_shapes=[
            pltpu.VMEM((STEPS, nj + 2, ni + 2, nk + 2 * TILE, lanes), f32),
            pltpu.VMEM((nj, ni, nk, lanes), f32),
            pltpu.VMEM((nj, ni, nk, lanes), f32),
            pltpu.VMEM((nj, ni, nk, lanes), f32),
            pltpu.VMEM((STEPS, 2, nj, ni, lanes), f32),
            pltpu.VMEM((STEPS, 2, nj, ni, lanes), f32),
            dma((nj + 2,)),
            dma((3, nj)),
            dma((STEPS, 2, nj)),
            dma((STEPS, 2, nj)),
            dma((STEPS, 2, nj)),
            dma((STEPS, 2, nj)),
            dma((STEPS, 2)),
            dma((STEPS, 2)),
        ],
        compiler_params=pltpu.CompilerParams(
            collective_id=0, has_side_effects=True, vmem_limit_bytes=58 * 1024 * 1024
        ),
    )(density, flow_j, flow_i, flow_k)


def solution(mesh):
    spec = P(("ens", "south"), "east", "down", None)
    counts = tuple(mesh.shape[a] for a in ("south", "east", "down"))
    return jax.shard_map(
        functools.partial(per_device, counts),
        mesh=mesh,
        in_specs=(spec,) * 4,
        out_specs=spec,
        check_vma=False,
    )
```
